768 devices in a mesh: shore: 24 (over z_hi, x, core), cross: 32 (over z_lo, y).
Axes of the slice: x: 4, y: 8, z: 12 (z_hi: 3, z_lo: 4; z = z_hi * 4 + z_lo), core: 2. Of those that a mesh axis runs over, the one named last changes fastest.
Arguments:
- positions: float32 [2, 384, 256, 128], P(None, 'shore', 'cross'), may hold values from 0 to 1
- velocity: float32 [2, 384, 256, 128], P(None, 'shore', 'cross'), may hold values from -3 to 3
- density: float32 [384, 256, 128], P('shore', 'cross'), may hold values from 0.97 to 1.03
- particle_mass: float32 [384, 256, 128], P('shore', 'cross'), may hold values from 0.004 to 0.016
- cell_count: int32 [384, 256], P('shore', 'cross'), may hold values from 0 to 128
- wind_seed: int32 [384, 256, 128], P('shore', 'cross'), may hold values from 0 to 15
- wind_table: float32 [2, 16], replicated, may hold values from -4 to 4
- migrant_slot: int32 [24, 32, 4, 1792], P('shore', 'cross'), may hold values from 0 to 16383
- migrant_count: int32 [24, 32, 4], P('shore', 'cross'), may hold values from 896 to 1792, as said below
Outputs:
- state_next: float32 [7, 384, 256, 128], P(None, 'shore', 'cross')
- arrivals: float32 [24, 32, 4, 8, 1792], P('shore', 'cross')
The draws below stay inside these ranges and needn't reach their ends.
Inputs may be any that keep to these rules, and one draw needn't show every extreme that they name: `migrant_slot`: a slot in one device's own blocks, numbered (block along * 8 + block across) * 128 + slot. `migrant_count`: on every device, at least one direction has exactly 1792 migrants.
All inputs are finite; a program needn't handle non-finite values.
Results may differ from the reference program's by a relative error of at most 0.0003.
Values sent between devices are 32-bit elements; how exact they have to be, the bound alone decides.
A program may use at most 32 MiB of HBM per device.

```python
import math
import jax
import jax.numpy as jnp
from jax import lax

CX = 16
CY = 8
P_SIZE = 128
LEVELS = 16
MIG = 1792
NCX = 384
NCY = 256
N_SHORE = 24
N_CROSS = 32


def draw_migrant_count(key, part):
    base = jax.random.randint(jax.random.fold_in(key, 11), (N_SHORE, N_CROSS, 4), MIG // 2, MIG + 1)
    full_dir = jax.random.randint(jax.random.fold_in(key, 12), (N_SHORE, N_CROSS, 1), 0, 4)
    directions = jnp.arange(4, dtype=jnp.int32)[None, None, :]
    return jnp.where(directions == full_dir, MIG, base).astype(jnp.int32)


def draw_cell_count(key, part):
    dense = jax.random.randint(jax.random.fold_in(key, 21), (NCX, NCY), P_SIZE // 2, P_SIZE + 1)
    sparse = jax.random.randint(jax.random.fold_in(key, 22), (NCX, NCY), 0, P_SIZE // 8 + 1)
    shore_device = jnp.arange(NCX, dtype=jnp.int32) // CX
    thin_reach = (shore_device >= N_SHORE - N_SHORE // 3)[:, None]
    return jnp.where(thin_reach, sparse, dense).astype(jnp.int32)


def place_ends(values, stream_key, smallest, top_value):
    longest = values.shape.index(max(values.shape))
    spots = []
    for shift in (0, 1):
        where = [jax.random.randint(jax.random.fold_in(stream_key, axis), (), 0, length) for axis, length in enumerate(values.shape)]
        where[longest] = (where[longest] + shift) % values.shape[longest]
        spots.append(tuple(where))
    return values.at[spots[0]].set(smallest).at[spots[1]].set(top_value)


def block_levels(own_key, dims, split, low, largest):
    gain = 1.0
    for dim, blocks in split:
        steps = jax.random.uniform(jax.random.fold_in(jax.random.fold_in(own_key, 6), dim), (blocks,), jnp.float32, low / len(split), largest / len(split))
        gain = gain * jnp.repeat(jnp.exp(steps), dims[dim] // blocks).reshape((-1,) + (1,) * (len(dims) - 1 - dim))
    return gain


def scatter_about(key, extent, scale, bound, shards=(), held_as=jnp.bfloat16):
    array = jax.random.normal(key, extent, jnp.float32) * scale
    if len(shards) > 0:
        array = block_levels(key, extent, shards, -0.22, 0.18) * array
    return jnp.clip(array, min=-bound, max=bound).astype(held_as)


def setup_inputs(seed: int = 0) -> dict:
    keys = jax.random.split(jax.random.key(seed), 10)
    positions = jnp.clip(1.0 * jax.random.uniform(keys[0], (2, NCX, NCY, P_SIZE), jnp.float32) ** block_levels(keys[0], (2, NCX, NCY, P_SIZE), ((1, 24), (2, 32)), -0.2, 0.2), 0.0, 1.0)
    velocity = scatter_about(keys[1], (2, NCX, NCY, P_SIZE), 0.5, 3.0, ((1, 24), (2, 32)), jnp.float32)
    density = jnp.clip(0.97 + 0.059999943 * jax.random.uniform(keys[2], (NCX, NCY, P_SIZE), jnp.float32) ** block_levels(keys[2], (NCX, NCY, P_SIZE), ((0, 24), (1, 32)), -0.2, 0.2), 0.97, 1.03)
    particle_mass = jnp.clip(jnp.exp(math.log(0.016) - 1.3862944 * jax.random.uniform(keys[3], (NCX, NCY, P_SIZE), jnp.float32) ** block_levels(keys[3], (NCX, NCY, P_SIZE), ((0, 24), (1, 32)), -0.2, 0.2)), 0.004, 0.016)
    cell_count = draw_cell_count(jax.random.fold_in(keys[9], 71), 0)
    wind_seed = place_ends(jax.random.randint(keys[5], (NCX, NCY, P_SIZE), 0, LEVELS), jax.random.fold_in(keys[5], 1), 0, LEVELS - 1).astype(jnp.int32)
    wind_table = scatter_about(keys[6], (2, LEVELS), 1.0, 4.0, (), jnp.float32)
    migrant_slot = place_ends(jax.random.randint(keys[7], (N_SHORE, N_CROSS, 4, MIG), 0, CX * CY * P_SIZE), jax.random.fold_in(keys[7], 1), 0, (CX * CY * P_SIZE) - 1).astype(jnp.int32)
    migrant_count = draw_migrant_count(jax.random.fold_in(keys[9], 71), 0)
    return dict(positions=positions, velocity=velocity, density=density, particle_mass=particle_mass, cell_count=cell_count, wind_seed=wind_seed, wind_table=wind_table, migrant_slot=migrant_slot, migrant_count=migrant_count)


sound_speed = 10.0
smooth = 0.5
viscous = 0.1
kernel_norm = 7.0 / (4.0 * 3.141592653589793 * smooth * smooth)
grad_coef = -5.0 * kernel_norm / (smooth * smooth)

def pressure_ratio(density):
    cube = density * density * density
    seventh = cube * cube * density
    pressure = sound_speed * sound_speed / 7.0 * (seventh - 1.0)
    return pressure / (density * density)

def pack_fields(positions, velocity, density, particle_mass, live_slots):
    return jnp.stack([positions[0], positions[1], velocity[0], velocity[1], density, particle_mass, live_slots, pressure_ratio(density)])

def tile_terms(own_cells, near_cells, step_x, step_y):
    offset_x = own_cells[0][:, :, None] - near_cells[0][:, None, :] - step_x
    offset_y = own_cells[1][:, :, None] - near_cells[1][:, None, :] - step_y
    dist_sq = offset_x * offset_x + offset_y * offset_y
    radius = jnp.sqrt(dist_sq) / smooth
    falloff = jnp.maximum(1.0 - 0.5 * radius, 0.0)
    gradient = grad_coef * falloff * falloff * falloff
    relative_u = own_cells[2][:, :, None] - near_cells[2][:, None, :]
    relative_v = own_cells[3][:, :, None] - near_cells[3][:, None, :]
    approach = relative_u * offset_x + relative_v * offset_y
    viscous_mu = smooth * jnp.minimum(approach, 0.0) / (dist_sq + 0.01 * smooth * smooth)
    mean_density = 0.5 * (own_cells[4][:, :, None] + near_cells[4][:, None, :])
    visc_term = -viscous * sound_speed * viscous_mu / mean_density
    weighted = (near_cells[5] * near_cells[6])[:, None, :] * gradient
    coupling = weighted * (own_cells[7][:, :, None] + near_cells[7][:, None, :] + visc_term)
    force_x = -lax.optimization_barrier(jnp.sum(coupling * offset_x, axis=2))
    force_y = -lax.optimization_barrier(jnp.sum(coupling * offset_y, axis=2))
    density_rate = lax.optimization_barrier(jnp.sum(weighted * approach, axis=2))
    return jnp.stack([force_x, force_y, density_rate])

def row_forces(three_rows):
    own_cells = three_rows[:, 1, 1:-1]
    width = own_cells.shape[1]
    summed = jnp.zeros((3,) + own_cells.shape[1:], jnp.float32)
    for step_x in (-1, 0, 1):
        for step_y in (-1, 0, 1):
            near_cells = three_rows[:, 1 + step_x, 1 + step_y:1 + step_y + width]
            summed = summed + tile_terms(own_cells, near_cells, float(step_x), float(step_y))
    return summed

def all_forces(extended):
    row_count = extended.shape[1] - 2

    def one_row(row_index):
        return row_forces(lax.dynamic_slice_in_dim(extended, row_index, 3, 1))
    computed = lax.map(one_row, jnp.arange(row_count, dtype=jnp.int32))
    return jnp.transpose(computed, (1, 0, 2, 3))

def time_step(peak_acc, peak_speed):
    return 0.25 * smooth / (sound_speed + peak_speed + jnp.sqrt(smooth * peak_acc))

def pick_migrants(flattened, slot_list, live_count):
    width = slot_list.shape[1]
    picked = jnp.take(flattened, slot_list.reshape(-1).astype(jnp.int32), axis=1)
    picked = jnp.transpose(picked.reshape(flattened.shape[0], 4, width), (1, 0, 2))
    live_rows = (jnp.arange(width, dtype=jnp.int32)[None, :] < live_count[:, None]).astype(jnp.float32)
    return picked * live_rows[:, None, :]

def reference(positions, velocity, density, particle_mass, cell_count, wind_seed, wind_table, migrant_slot, migrant_count):
    slot_ids = jnp.arange(P_SIZE, dtype=jnp.int32)
    live_slots = (slot_ids[None, None, :] < cell_count[:, :, None]).astype(jnp.float32)
    fields = pack_fields(positions, velocity, density, particle_mass, live_slots)
    extended = jnp.pad(fields, ((0, 0), (1, 1), (1, 1), (0, 0)))
    forces = all_forces(extended)
    windage = wind_table[:, wind_seed]
    acceleration = (forces[:2] + windage) * live_slots[None]
    density_rate = forces[2] * live_slots
    peak_acc = jnp.max(jnp.sqrt(acceleration[0] * acceleration[0] + acceleration[1] * acceleration[1]))
    peak_speed = jnp.max(jnp.sqrt(velocity[0] * velocity[0] + velocity[1] * velocity[1]) * live_slots)
    delta_t = time_step(peak_acc, peak_speed)
    new_velocity = (velocity + delta_t * acceleration) * live_slots[None]
    new_position = (positions + delta_t * new_velocity) * live_slots[None]
    new_density = (density + delta_t * density_rate) * live_slots
    state_next = jnp.concatenate([new_position, new_velocity, new_density[None], acceleration])
    carried = jnp.concatenate([new_position, new_velocity, new_density[None], (particle_mass * live_slots)[None], acceleration])
    per_device = carried.reshape(8, N_SHORE, CX, N_CROSS, CY, P_SIZE)
    per_device = jnp.transpose(per_device, (1, 3, 0, 2, 4, 5)).reshape(N_SHORE, N_CROSS, 8, CX * CY * P_SIZE)
    leaving = jax.vmap(jax.vmap(pick_migrants))(per_device, migrant_slot, migrant_count)
    zero_shore = jnp.zeros_like(leaving[:1, :, 0])
    eastward = jnp.concatenate([zero_shore, leaving[:-1, :, 0]], axis=0)
    westward = jnp.concatenate([leaving[1:, :, 1], zero_shore], axis=0)
    zero_cross = jnp.zeros_like(leaving[:, :1, 2])
    northward = jnp.concatenate([zero_cross, leaving[:, :-1, 2]], axis=1)
    southward = jnp.concatenate([leaving[:, 1:, 3], zero_cross], axis=1)
    arrivals = jnp.stack([eastward, westward, northward, southward], axis=2)
    return (state_next, arrivals)
```

```python
import functools

import jax
import jax.numpy as jnp
from jax import lax
from jax.experimental import pallas as pl
from jax.experimental.pallas import tpu as pltpu
from jax.sharding import PartitionSpec as P

MESH = pl.DeviceIdType.MESH
SUB, LANES = 8, 128
GROUP = 2
FIELDS = 7
TILE = 256
TINY = 1e-30

sound_speed = 10.0
smooth = 0.5
viscous = 0.1
kernel_norm = 7.0 / (4.0 * 3.141592653589793 * smooth * smooth)
grad_coef = -5.0 * kernel_norm / (smooth * smooth)


def pressure_ratio(density):
    cube = density * density * density
    seventh = cube * cube * density
    pressure = sound_speed * sound_speed / 7.0 * (seventh - 1.0)
    return pressure / (density * density)


def padded(cells, sides):
    for axis, dim in sides:
        ends = lax.axis_size(axis) - 1
        head = lax.slice_in_dim(cells, 0, 1, axis=dim)
        tail = lax.slice_in_dim(cells, cells.shape[dim] - 1, cells.shape[dim], axis=dim)
        cells = jnp.concatenate(
            [
                lax.ppermute(tail, axis, [(i, i + 1) for i in range(ends)]),
                cells,
                lax.ppermute(head, axis, [(i + 1, i) for i in range(ends)]),
            ],
            axis=dim,
        )
    return cells


def halves(exact, parts):
    got = []
    for _ in range(parts):
        got.append(exact.astype(jnp.bfloat16))
        exact = exact - got[-1].astype(jnp.float32)
    return got


def force_kernel(
    counts_ref, table_ref, cells_ref, pick_ref, seed_ref, live_ref, base_ref, out_ref, peak_ref, placed, wide, sums
):
    height, width = cells_ref.shape[:2]
    rows, cols = height - 2, width - 2
    field = lax.broadcasted_iota(jnp.int32, (SUB, LANES), 0)

    @pl.loop(0, height)
    def _(row):
        for col in range(width):
            shift = jnp.where(field == 0, row.astype(jnp.float32), jnp.where(field == 1, float(col), 0.0))
            placed[row, col] = cells_ref[row, col] + shift

    @pl.loop(0, rows)
    def _(row):
        for col in range(cols):
            for c in range(3):
                sums[row, col, c] = jnp.zeros((SUB, LANES), jnp.float32)

    def widen(row):
        for col in range(width):
            split = jnp.concatenate([x.astype(jnp.float32) for x in halves(placed[row, col], 3)], axis=0)
            wide[col] = lax.dot_general(
                jnp.transpose(split).astype(jnp.bfloat16),
                pick_ref[...],
                (((1,), (0,)), ((), ())),
                preferred_element_type=jnp.float32,
            )

    def one_cell(row, col, row_steps, col_steps):
        count = lax.div(counts_ref[row, col] + (SUB * GROUP - 1), SUB * GROUP)

        @pl.loop(0, count)
        def _(part):
            near = []
            for g in range(GROUP):
                at = pl.ds(pl.multiple_of((part * GROUP + g) * SUB, SUB), SUB)
                near.append(tuple(wide[col, at, f * LANES : (f + 1) * LANES] for f in range(FIELDS)))
            for dr in row_steps:
                for dc in col_steps:
                    xi, yi, ui, vi, di, pi = (
                        jnp.broadcast_to(placed[row + dr, col + dc, f : f + 1, :], (SUB, LANES)) for f in range(6)
                    )
                    fx = fy = rate = None
                    for g in range(GROUP):
                        xj, yj, uj, vj, dj, pj, mj = near[g]
                        ox = xi - xj
                        oy = yi - yj
                        d2 = ox * ox + oy * oy
                        r = d2 * lax.rsqrt(jnp.maximum(d2, TINY))
                        f = jnp.maximum(1.0 - r, 0.0)
                        w = mj * (f * f * f)
                        a = (ui - uj) * ox + (vi - vj) * oy
                        q = (d2 + 0.01 * smooth * smooth) * (di + dj)
                        c = w * ((pi + pj) - jnp.minimum(a, 0.0) * pl.reciprocal(q))
                        fx = c * ox if g == 0 else fx + c * ox
                        fy = c * oy if g == 0 else fy + c * oy
                        rate = w * a if g == 0 else rate + w * a
                    own = (row + dr - 1, col + dc - 1)
                    sums[own[0], own[1], 0] += fx
                    sums[own[0], own[1], 1] += fy
                    sums[own[0], own[1], 2] += rate

    def one_row(row, row_steps):
        widen(row)
        one_cell(row, 0, row_steps, (1,))
        one_cell(row, 1, row_steps, (0, 1))

        @pl.loop(2, width - 2)
        def _(col):
            one_cell(row, col, row_steps, (-1, 0, 1))

        one_cell(row, width - 2, row_steps, (-1, 0))
        one_cell(row, width - 1, row_steps, (-1,))

    one_row(0, (1,))
    one_row(1, (0, 1))

    @pl.loop(2, height - 2)
    def _(row):
        one_row(row, (-1, 0, 1))

    one_row(height - 2, (-1, 0))
    one_row(height - 1, (-1,))

    def finish(row, peaks):
        live = live_ref[row]
        seed = seed_ref[row]
        got = []
        for c in range(3):
            got.append(
                jnp.concatenate(
                    [jnp.sum(sums[row, col, c], axis=0, keepdims=True) for col in range(cols)], axis=0
                )
            )
        acc = []
        for c in range(2):
            wind = jnp.full(seed.shape, table_ref[c, 0], jnp.float32)
            for level in range(1, table_ref.shape[1]):
                wind = jnp.where(seed == level, table_ref[c, level], wind)
            acc.append((wind - got[c]) * live)
            out_ref[c, row] = acc[c]
        out_ref[2, row] = got[2] * live
        vx, vy = base_ref[2, row], base_ref[3, row]
        return (
            jnp.maximum(peaks[0], acc[0] * acc[0] + acc[1] * acc[1]),
            jnp.maximum(peaks[1], vx * vx + vy * vy),
        )

    zero = jnp.zeros((cols, LANES), jnp.float32)
    peaks = lax.fori_loop(0, rows, finish, (zero, zero))
    peak_ref[...] = jnp.where(field < 4, jnp.max(peaks[0]), jnp.max(peaks[1]))


def all_forces(counts, table, cells, seed, live, base):
    height, width = cells.shape[:2]
    rows, cols = height - 2, width - 2
    which = lax.broadcasted_iota(jnp.int32, (24, FIELDS * LANES), 0) % 8
    pick = (which == lax.broadcasted_iota(jnp.int32, (24, FIELDS * LANES), 1) // LANES).astype(jnp.bfloat16)
    return pl.pallas_call(
        force_kernel,
        out_shape=(
            jax.ShapeDtypeStruct((3, rows, cols, LANES), jnp.float32),
            jax.ShapeDtypeStruct((SUB, LANES), jnp.float32),
        ),
        in_specs=[pl.BlockSpec(memory_space=pltpu.SMEM)] * 2 + [pl.BlockSpec(memory_space=pltpu.VMEM)] * 5,
        out_specs=(pl.BlockSpec(memory_space=pltpu.VMEM),) * 2,
        scratch_shapes=[
            pltpu.VMEM((height, width, SUB, LANES), jnp.float32),
            pltpu.VMEM((width, LANES, FIELDS * LANES), jnp.float32),
            pltpu.VMEM((rows, cols, 3, SUB, LANES), jnp.float32),
        ],
        compiler_params=pltpu.CompilerParams(vmem_limit_bytes=32 << 20),
    )(counts, table, cells, pick, seed, live, base)


def exchange_kernel(
    groups, counts_ref, slots_ref, base_ref, moved_ref, peak_ref, got_ref, top_ref,
    split, leaving, held, heap_a, heap_b, heap_c, send_a, recv_a, send_b, recv_b, send_c, recv_c, send_m, recv_m,
):
    inner, outer, near, far = groups
    shore, cross = lax.axis_index("shore"), lax.axis_index("cross")
    shores, crosses = inner * outer, near * far
    s_out, s_in = lax.div(shore, inner), lax.rem(shore, inner)
    c_out, c_in = lax.div(cross, near), lax.rem(cross, near)

    along = [
        (s_out * inner + lax.rem(s_in + o, inner), cross) for o in range(1, inner)
    ]
    across = [(shore, c_out * near + lax.rem(c_in + o, near)) for o in range(1, near)]
    depth = []
    for o in range(1, outer * far):
        spot = lax.rem(s_out * far + c_out + o, outer * far)
        depth.append((lax.div(spot, far) * inner + s_in, lax.rem(spot, far) * near + c_in))
    ends = [
        (shore < shores - 1, shore > 0, (shore + 1, cross)),
        (shore > 0, shore < shores - 1, (shore - 1, cross)),
        (cross < crosses - 1, cross > 0, (shore, cross + 1)),
        (cross > 0, cross < crosses - 1, (shore, cross - 1)),
    ]

    barrier = pltpu.get_barrier_semaphore()
    beside = [
        (lax.rem(shore + 1, shores), cross),
        (lax.rem(shore + shores - 1, shores), cross),
        (shore, lax.rem(cross + 1, crosses)),
        (shore, lax.rem(cross + crosses - 1, crosses)),
    ]
    greeted = along + across + depth + beside
    for peer in greeted:
        pl.semaphore_signal(barrier, inc=1, device_id=peer, device_id_type=MESH)

    kinds = base_ref.shape[0] + moved_ref.shape[0]
    cells = base_ref.shape[1] * base_ref.shape[2]
    for f in range(kinds):
        source = base_ref[f] if f < base_ref.shape[0] else moved_ref[f - base_ref.shape[0]]
        high, low = halves(source.reshape(cells, LANES), 2)
        split[f * cells : (f + 1) * cells, 0:LANES] = high
        split[f * cells : (f + 1) * cells, LANES : 2 * LANES] = low

    width = slots_ref.shape[1]
    rank = lax.broadcasted_iota(jnp.int32, (LANES, TILE), 0)
    for d in range(4):

        @pl.loop(0, width // TILE)
        def _(t):
            at = pl.ds(pl.multiple_of(t * TILE, TILE), TILE)
            slot = slots_ref[d : d + 1, at]
            lane = jnp.where(rank == (slot & (LANES - 1)), 1.0, 0.0)
            lanes = jnp.concatenate([lane, lane], axis=0).astype(jnp.bfloat16)
            order = lax.broadcasted_iota(jnp.int32, (1, TILE), 1) + t * TILE
            cell = jnp.where(order < counts_ref[d], lax.shift_right_logical(slot, 7), -1)
            keep = rank == cell
            for f in range(kinds):
                found = jnp.dot(
                    split[f * cells : (f + 1) * cells, :], lanes, preferred_element_type=jnp.float32
                )
                leaving[d, f : f + 1, at] = jnp.sum(jnp.where(keep, found, 0.0), axis=0, keepdims=True)

    pl.semaphore_wait(barrier, len(greeted))

    def migrants(d):
        return pltpu.make_async_remote_copy(
            src_ref=leaving.at[d],
            dst_ref=got_ref.at[d],
            send_sem=send_m.at[d],
            recv_sem=recv_m.at[d],
            device_id=ends[d][2],
            device_id_type=MESH,
        )

    held[0] = peak_ref[...]
    stages = ((along, heap_a, send_a, recv_a), (across, heap_b, send_b, recv_b), (depth, heap_c, send_c, recv_c))
    for step, (peers, heap, send, recv) in enumerate(stages):
        copies = [
            pltpu.make_async_remote_copy(
                src_ref=held.at[step],
                dst_ref=heap.at[o],
                send_sem=send.at[o],
                recv_sem=recv.at[o],
                device_id=peer,
                device_id_type=MESH,
            )
            for o, peer in enumerate(peers)
        ]
        for copy in copies:
            copy.start()
        if step == 0:
            for d in range(4):

                @pl.when(ends[d][0])
                def _():
                    migrants(d).start()

        top = held[step]
        for o, copy in enumerate(copies):
            copy.wait()
            top = jnp.maximum(top, heap[o])
        held[step + 1] = top
    top_ref[...] = held[len(stages)]

    for d in range(4):

        @pl.when(ends[d][0])
        def _():
            migrants(d).wait_send()

        @pl.when(ends[d][1])
        def _():
            migrants(d).wait_recv()

        @pl.when(jnp.logical_not(ends[d][1]))
        def _():
            got_ref[d] = jnp.zeros(got_ref.shape[1:], jnp.float32)


def exchange(groups, counts, slots, base, moved, peak):
    inner, outer, near, far = groups
    kinds = base.shape[0] + moved.shape[0]
    cells = base.shape[1] * base.shape[2]
    width = slots.shape[1]
    dma = pltpu.SemaphoreType.DMA
    sems = []
    for peers in (inner - 1, near - 1, outer * far - 1, 4):
        sems += [dma((peers,)), dma((peers,))]
    return pl.pallas_call(
        functools.partial(exchange_kernel, groups),
        out_shape=(
            jax.ShapeDtypeStruct((4, kinds, width), jnp.float32),
            jax.ShapeDtypeStruct((SUB, LANES), jnp.float32),
        ),
        in_specs=[pl.BlockSpec(memory_space=pltpu.SMEM)] + [pl.BlockSpec(memory_space=pltpu.VMEM)] * 4,
        out_specs=(pl.BlockSpec(memory_space=pltpu.VMEM),) * 2,
        scratch_shapes=[
            pltpu.VMEM((kinds * cells, 2 * LANES), jnp.bfloat16),
            pltpu.VMEM((4, kinds, width), jnp.float32),
            pltpu.VMEM((4, SUB, LANES), jnp.float32),
            pltpu.VMEM((inner - 1, SUB, LANES), jnp.float32),
            pltpu.VMEM((near - 1, SUB, LANES), jnp.float32),
            pltpu.VMEM((outer * far - 1, SUB, LANES), jnp.float32),
        ]
        + sems,
        compiler_params=pltpu.CompilerParams(collective_id=0, has_side_effects=True),
    )(counts, slots, base, moved, peak)


def advance_kernel(top_ref, base_ref, moved_ref, got_ref, state_ref, arrivals_ref):
    peak_acc = jnp.sqrt(jnp.max(top_ref[0:4], axis=(0, 1), keepdims=True))
    peak_speed = jnp.sqrt(jnp.max(top_ref[4:8], axis=(0, 1), keepdims=True))
    step = 0.25 * smooth / (sound_speed + peak_speed + jnp.sqrt(smooth * peak_acc))
    for c in range(2):
        speed = base_ref[2 + c] + step * moved_ref[c]
        state_ref[2 + c] = speed
        state_ref[c] = base_ref[c] + step * speed
        state_ref[5 + c] = moved_ref[c]
    state_ref[4] = base_ref[4] + step * moved_ref[2]
    for d in range(4):
        for c in range(2):
            push = got_ref[d, 6 + c : 7 + c]
            speed = got_ref[d, 2 + c : 3 + c] + step * push
            arrivals_ref[0, 0, d, 2 + c : 3 + c] = speed
            arrivals_ref[0, 0, d, c : c + 1] = got_ref[d, c : c + 1] + step * speed
            arrivals_ref[0, 0, d, 6 + c : 7 + c] = push
        arrivals_ref[0, 0, d, 4:5] = got_ref[d, 4:5] + step * got_ref[d, 8:9]
        arrivals_ref[0, 0, d, 5:6] = got_ref[d, 5:6]


def advance(top, base, moved, got):
    return pl.pallas_call(
        advance_kernel,
        out_shape=(
            jax.ShapeDtypeStruct((7,) + base.shape[1:], jnp.float32),
            jax.ShapeDtypeStruct((1, 1, 4, 8, got.shape[2]), jnp.float32),
        ),
        in_specs=[pl.BlockSpec(memory_space=pltpu.VMEM)] * 4,
        out_specs=(pl.BlockSpec(memory_space=pltpu.VMEM),) * 2,
    )(top, base, moved, got)


def body(
    groups, positions, velocity, density, particle_mass, cell_count, wind_seed, wind_table, migrant_slot, migrant_count
):
    slot_ids = jnp.arange(positions.shape[3], dtype=jnp.int32)
    live = (slot_ids[None, None, :] < cell_count[:, :, None]).astype(jnp.float32)
    base = jnp.concatenate(
        [positions * live, velocity * live, (density * live)[None], (particle_mass * live)[None]]
    )
    cells = jnp.stack(
        [
            positions[0],
            positions[1],
            velocity[0],
            velocity[1],
            density,
            pressure_ratio(density),
            grad_coef * (particle_mass * live),
            live,
        ],
        axis=2,
    )
    cells = padded(cells, (("shore", 0), ("cross", 1)))
    counts = jnp.sum(cells[:, :, 7, :], axis=2).astype(jnp.int32)
    moved, peak = all_forces(counts, wind_table, cells, wind_seed, live, base)
    got, top = exchange(groups, migrant_count[0, 0], migrant_slot[0, 0], base, moved, peak)
    return advance(top, base, moved, got)


def solution(mesh):
    shores, crosses = mesh.shape["shore"], mesh.shape["cross"]
    groups = (8, shores // 8, 8, crosses // 8)
    lined = P("shore", "cross", None)
    return jax.shard_map(
        functools.partial(body, groups),
        mesh=mesh,
        in_specs=(
            P(None, "shore", "cross", None),
            P(None, "shore", "cross", None),
            lined,
            lined,
            P("shore", "cross"),
            lined,
            P(),
            P("shore", "cross", None, None),
            lined,
        ),
        out_specs=(P(None, "shore", "cross", None), P("shore", "cross", None, None, None)),
        check_vma=False,
    )
```

```python
import functools

import jax
import jax.numpy as jnp
from jax import lax
from jax.experimental import pallas as pl
from jax.experimental.pallas import tpu as pltpu
from jax.sharding import PartitionSpec as P

MESH = pl.DeviceIdType.MESH
SUB, LANES = 8, 128
GROUP = 2
FIELDS = 7
TILE = 256
TINY = 1e-30

sound_speed = 10.0
smooth = 0.5
viscous = 0.1
kernel_norm = 7.0 / (4.0 * 3.141592653589793 * smooth * smooth)
grad_coef = -5.0 * kernel_norm / (smooth * smooth)


def pressure_ratio(density):
    cube = density * density * density
    seventh = cube * cube * density
    pressure = sound_speed * sound_speed / 7.0 * (seventh - 1.0)
    return pressure / (density * density)


def halo_kernel(
    shores, crosses, count_ref, positions_ref, velocity_ref, density_ref, mass_ref, cells_ref, base_ref, live_ref, send, recv
):
    shore, cross = lax.axis_index("shore"), lax.axis_index("cross")
    rows, cols = live_ref.shape[:2]
    steps = [(dx, dy) for dx in (-1, 0, 1) for dy in (-1, 0, 1) if dx or dy]
    barrier = pltpu.get_barrier_semaphore()
    for dx, dy in steps:
        peer = (lax.rem(shore + dx + shores, shores), lax.rem(cross + dy + crosses, crosses))
        pl.semaphore_signal(barrier, inc=1, device_id=peer, device_id_type=MESH)

    which = lax.broadcasted_iota(jnp.int32, (cols, LANES), 0)
    slot = lax.broadcasted_iota(jnp.int32, (cols, LANES), 1)

    @pl.loop(0, rows)
    def _(row):
        filled = jnp.full((cols, LANES), count_ref[row, 0], jnp.int32)
        for col in range(1, cols):
            filled = jnp.where(which == col, count_ref[row, col], filled)
        live = jnp.where(slot < filled, 1.0, 0.0)
        x, y, u, v = positions_ref[0, row], positions_ref[1, row], velocity_ref[0, row], velocity_ref[1, row]
        dense = density_ref[row]
        mass = mass_ref[row] * live
        fields = (x, y, u, v, dense, pressure_ratio(dense), grad_coef * mass, live)
        for f, value in enumerate(fields):
            cells_ref[row + 1, 1 : cols + 1, f, :] = value
        for f, value in enumerate((x * live, y * live, u * live, v * live, dense * live, mass)):
            base_ref[f, row] = value
        live_ref[row] = live

    pl.semaphore_wait(barrier, len(steps))

    def edge(step, count):
        return pl.ds(1, count) if step == 0 else pl.ds(1 if step < 0 else count, 1)

    def rim(step, count):
        return pl.ds(1, count) if step == 0 else pl.ds(count + 1 if step < 0 else 0, 1)

    def inside(dx, dy):
        found = True
        for at, step, ends in ((shore, dx, shores), (cross, dy, crosses)):
            if step:
                found = jnp.logical_and(found, at < ends - 1 if step > 0 else at > 0)
        return found

    def copy(k):
        dx, dy = steps[k]
        return pltpu.make_async_remote_copy(
            src_ref=cells_ref.at[edge(dx, rows), edge(dy, cols)],
            dst_ref=cells_ref.at[rim(dx, rows), rim(dy, cols)],
            send_sem=send.at[k],
            recv_sem=recv.at[k],
            device_id=(shore + dx, cross + dy),
            device_id_type=MESH,
        )

    for k, (dx, dy) in enumerate(steps):

        @pl.when(inside(dx, dy))
        def _():
            copy(k).start()

    for k, (dx, dy) in enumerate(steps):

        @pl.when(jnp.logical_not(inside(-dx, -dy)))
        def _():
            at = (rim(dx, rows), rim(dy, cols))
            cells_ref[at] = jnp.zeros((at[0].size, at[1].size, SUB, LANES), jnp.float32)

    for k, (dx, dy) in enumerate(steps):

        @pl.when(inside(dx, dy))
        def _():
            copy(k).wait_send()

        @pl.when(inside(-dx, -dy))
        def _():
            copy(k).wait_recv()


def halo(shores, crosses, cell_count, positions, velocity, density, particle_mass):
    rows, cols = density.shape[:2]
    vmem = pl.BlockSpec(memory_space=pltpu.VMEM)
    return pl.pallas_call(
        functools.partial(halo_kernel, shores, crosses),
        out_shape=(
            jax.ShapeDtypeStruct((rows + 2, cols + 2, SUB, LANES), jnp.float32),
            jax.ShapeDtypeStruct((6, rows, cols, LANES), jnp.float32),
            jax.ShapeDtypeStruct((rows, cols, LANES), jnp.float32),
        ),
        in_specs=[pl.BlockSpec(memory_space=pltpu.SMEM)] + [vmem] * 4,
        out_specs=(vmem,) * 3,
        scratch_shapes=[pltpu.SemaphoreType.DMA((8,)), pltpu.SemaphoreType.DMA((8,))],
        compiler_params=pltpu.CompilerParams(collective_id=1, has_side_effects=True),
    )(cell_count, positions, velocity, density, particle_mass)


def halves(exact, parts):
    got = []
    for _ in range(parts):
        got.append(exact.astype(jnp.bfloat16))
        exact = exact - got[-1].astype(jnp.float32)
    return got


def force_kernel(
    counts_ref, table_ref, cells_ref, pick_ref, seed_ref, live_ref, base_ref, out_ref, peak_ref, placed, wide, sums, returned
):
    height, width = cells_ref.shape[:2]
    rows, cols = height - 2, width - 2
    field = lax.broadcasted_iota(jnp.int32, (SUB, LANES), 0)

    @pl.loop(0, height)
    def _(row):
        for col in range(width):
            shift = jnp.where(field == 0, row.astype(jnp.float32), jnp.where(field == 1, float(col), 0.0))
            placed[row, col] = cells_ref[row, col] + shift

    @pl.loop(0, rows)
    def _(row):
        for col in range(cols):
            for c in range(3):
                sums[row, col, c] = jnp.zeros((SUB, LANES), jnp.float32)

    def widen(row):
        for col in range(width):
            split = jnp.concatenate([x.astype(jnp.float32) for x in halves(placed[row, col], 3)], axis=0)
            wide[col] = lax.dot_general(
                jnp.transpose(split).astype(jnp.bfloat16),
                pick_ref[...],
                (((1,), (0,)), ((), ())),
                preferred_element_type=jnp.float32,
            )

    def loop_over(row, col):
        count = lax.div(counts_ref[row, col] + (SUB * GROUP - 1), SUB * GROUP)

        def loaded(part):
            near = []
            for g in range(GROUP):
                at = pl.ds(pl.multiple_of((part * GROUP + g) * SUB, SUB), SUB)
                near.append(tuple(wide[col, at, f * LANES : (f + 1) * LANES] for f in range(FIELDS)))
            return near

        return count, loaded

    def shared(own, near):
        xi, yi, ui, vi, di, pi = own
        xj, yj, uj, vj, dj, pj = near
        ox = xi - xj
        oy = yi - yj
        d2 = ox * ox + oy * oy
        near_d2 = jnp.clip(d2, TINY, 1.0)
        f = 1.0 - near_d2 * lax.rsqrt(near_d2)
        f3 = f * f * f
        a = (ui - uj) * ox + (vi - vj) * oy
        q = (d2 + 0.01 * smooth * smooth) * (di + dj)
        return ox, oy, f3, a, (pi + pj) - jnp.minimum(a, 0.0) * pl.reciprocal(q)

    def row_of(row, col, f):
        return jnp.broadcast_to(placed[row, col, f : f + 1, :], (SUB, LANES))

    def plus(total, terms):
        return terms if total is None else tuple(t + x for t, x in zip(total, terms))

    def one_way(row, col, step, near):
        own = (row + step[0], col + step[1])
        fields = [row_of(own[0], own[1], f) for f in range(6)]
        total = None
        for there in near:
            ox, oy, f3, a, c = shared(fields, there[:6])
            w = there[6] * f3
            c = w * c
            total = plus(total, (c * ox, c * oy, w * a))
        for k in range(3):
            sums[own[0] - 1, own[1] - 1, k] += total[k]

    def both_ways(row, col, step, near, back):
        own = (row + step[0], col + step[1])
        fields = [row_of(own[0], own[1], f) for f in range(6)]
        mass = row_of(own[0], own[1], 6)
        total = None
        for g, there in enumerate(near):
            ox, oy, f3, a, c = shared(fields, there[:6])
            c = f3 * c
            terms = (c * ox, c * oy, f3 * a)
            total = plus(total, tuple(there[6] * t for t in terms))
            back[g] = plus(back[g], tuple(mass * t for t in terms))
        for k in range(3):
            sums[own[0] - 1, own[1] - 1, k] += total[k]

    def outer_cell(row, col, steps):
        count, loaded = loop_over(row, col)

        @pl.loop(0, count)
        def _(part):
            near = loaded(part)
            for step in steps:
                one_way(row, col, step, near)

    def inner_cell(row, col, steps):
        count, loaded = loop_over(row, col)

        @pl.loop(0, count)
        def _(part):
            near = loaded(part)
            back = [None] * GROUP
            one_way(row, col, (0, 0), near)
            for step in steps:
                both_ways(row, col, step, near, back)
            for g in range(GROUP):
                if back[g] is not None:
                    at = pl.ds(pl.multiple_of((part * GROUP + g) * SUB, SUB), SUB)
                    for k in range(3):
                        returned[col - 1, k, at, :] = back[g][k]

    def outer_row(row, step):
        widen(row)
        outer_cell(row, 0, ((step, 1),))
        outer_cell(row, 1, ((step, 0), (step, 1)))

        @pl.loop(2, width - 2)
        def _(col):
            outer_cell(row, col, ((step, -1), (step, 0), (step, 1)))

        outer_cell(row, width - 2, ((step, -1), (step, 0)))
        outer_cell(row, width - 1, ((step, -1),))

    def inner_row(row, drs, last):
        widen(row)
        outer_cell(row, 0, tuple((dr, 1) for dr in drs))
        outer_cell(row, width - 1, tuple((dr, -1) for dr in drs))
        down = () if last else ((1, -1), (1, 0), (1, 1))
        inner_cell(row, 1, ((0, 1),) + down[1:])

        @pl.loop(2, width - 2)
        def _(col):
            inner_cell(row, col, ((0, 1),) + down)

        inner_cell(row, width - 2, down[:2])
        for col in range(cols - 1 if last else cols):
            for k in range(3):
                turned = jnp.transpose(returned[col, k])
                total = turned[0:SUB]
                for v in range(1, LANES // SUB):
                    total = total + turned[v * SUB : (v + 1) * SUB]
                sums[row - 1, col, k] += total if k == 2 else -total

    @pl.loop(0, cols)
    def _(col):
        for k in range(3):
            returned[col, k] = jnp.zeros((LANES, LANES), jnp.float32)

    outer_row(0, 1)
    inner_row(1, (0, 1), False)

    @pl.loop(2, height - 2)
    def _(row):
        inner_row(row, (-1, 0, 1), False)

    inner_row(height - 2, (-1, 0), True)
    outer_row(height - 1, -1)

    def finish(row, peaks):
        live = live_ref[row]
        seed = seed_ref[row]
        got = []
        for c in range(3):
            got.append(
                jnp.concatenate(
                    [jnp.sum(sums[row, col, c], axis=0, keepdims=True) for col in range(cols)], axis=0
                )
            )
        acc = []
        for c in range(2):
            wind = jnp.full(seed.shape, table_ref[c, 0], jnp.float32)
            for level in range(1, table_ref.shape[1]):
                wind = jnp.where(seed == level, table_ref[c, level], wind)
            acc.append((wind - got[c]) * live)
            out_ref[c, row] = acc[c]
        out_ref[2, row] = got[2] * live
        vx, vy = base_ref[2, row], base_ref[3, row]
        return (
            jnp.maximum(peaks[0], acc[0] * acc[0] + acc[1] * acc[1]),
            jnp.maximum(peaks[1], vx * vx + vy * vy),
        )

    zero = jnp.zeros((cols, LANES), jnp.float32)
    peaks = lax.fori_loop(0, rows, finish, (zero, zero))
    peak_ref[...] = jnp.where(field < 4, jnp.max(peaks[0]), jnp.max(peaks[1]))


def all_forces(counts, table, cells, seed, live, base):
    height, width = cells.shape[:2]
    rows, cols = height - 2, width - 2
    which = lax.broadcasted_iota(jnp.int32, (24, FIELDS * LANES), 0) % 8
    pick = (which == lax.broadcasted_iota(jnp.int32, (24, FIELDS * LANES), 1) // LANES).astype(jnp.bfloat16)
    return pl.pallas_call(
        force_kernel,
        out_shape=(
            jax.ShapeDtypeStruct((3, rows, cols, LANES), jnp.float32),
            jax.ShapeDtypeStruct((SUB, LANES), jnp.float32),
        ),
        in_specs=[pl.BlockSpec(memory_space=pltpu.SMEM)] * 2 + [pl.BlockSpec(memory_space=pltpu.VMEM)] * 5,
        out_specs=(pl.BlockSpec(memory_space=pltpu.VMEM),) * 2,
        scratch_shapes=[
            pltpu.VMEM((height, width, SUB, LANES), jnp.float32),
            pltpu.VMEM((width, LANES, FIELDS * LANES), jnp.float32),
            pltpu.VMEM((rows, cols, 3, SUB, LANES), jnp.float32),
            pltpu.VMEM((cols, 3, LANES, LANES), jnp.float32),
        ],
        compiler_params=pltpu.CompilerParams(vmem_limit_bytes=32 << 20),
    )(counts, table, cells, pick, seed, live, base)


def exchange_kernel(
    groups, counts_ref, slots_ref, base_ref, moved_ref, peak_ref, got_ref, top_ref,
    split, found, leaving, held, heap_a, heap_b, heap_c, send_a, recv_a, send_b, recv_b, send_c, recv_c, send_m, recv_m,
):
    inner, outer, near, far = groups
    shore, cross = lax.axis_index("shore"), lax.axis_index("cross")
    shores, crosses = inner * outer, near * far
    s_out, s_in = lax.div(shore, inner), lax.rem(shore, inner)
    c_out, c_in = lax.div(cross, near), lax.rem(cross, near)

    along = [
        (s_out * inner + lax.rem(s_in + o, inner), cross) for o in range(1, inner)
    ]
    across = [(shore, c_out * near + lax.rem(c_in + o, near)) for o in range(1, near)]
    depth = []
    for o in range(1, outer * far):
        spot = lax.rem(s_out * far + c_out + o, outer * far)
        depth.append((lax.div(spot, far) * inner + s_in, lax.rem(spot, far) * near + c_in))
    ends = [
        (shore < shores - 1, shore > 0, (shore + 1, cross)),
        (shore > 0, shore < shores - 1, (shore - 1, cross)),
        (cross < crosses - 1, cross > 0, (shore, cross + 1)),
        (cross > 0, cross < crosses - 1, (shore, cross - 1)),
    ]

    barrier = pltpu.get_barrier_semaphore()
    beside = [
        (lax.rem(shore + 1, shores), cross),
        (lax.rem(shore + shores - 1, shores), cross),
        (shore, lax.rem(cross + 1, crosses)),
        (shore, lax.rem(cross + crosses - 1, crosses)),
    ]
    greeted = along + across + depth + beside
    for peer in greeted:
        pl.semaphore_signal(barrier, inc=1, device_id=peer, device_id_type=MESH)

    kinds = base_ref.shape[0] + moved_ref.shape[0]
    cells = base_ref.shape[1] * base_ref.shape[2]
    for f in range(kinds):
        source = base_ref[f] if f < base_ref.shape[0] else moved_ref[f - base_ref.shape[0]]
        high, low = halves(source.reshape(cells, LANES), 2)
        split[f * cells : (f + 1) * cells, 0:LANES] = high
        split[f * cells : (f + 1) * cells, LANES : 2 * LANES] = low

    width = slots_ref.shape[1]
    rank = lax.broadcasted_iota(jnp.int32, (LANES, TILE), 0)

    def gather(d):
        @pl.loop(0, width // TILE)
        def _(t):
            at = pl.ds(pl.multiple_of(t * TILE, TILE), TILE)
            slot = slots_ref[d : d + 1, at]
            lane = jnp.where(rank == (slot & (LANES - 1)), 1.0, 0.0)
            lanes = jnp.concatenate([lane, lane], axis=0).astype(jnp.bfloat16)
            found[...] = jnp.dot(split[...], lanes, preferred_element_type=jnp.float32)
            order = lax.broadcasted_iota(jnp.int32, (1, TILE), 1) + t * TILE
            cell = jnp.where(order < counts_ref[d], lax.shift_right_logical(slot, 7), -1)
            keep = rank == cell
            for f in range(kinds):
                mine = found[f * cells : (f + 1) * cells, :]
                leaving[d, f : f + 1, at] = jnp.sum(jnp.where(keep, mine, 0.0), axis=0, keepdims=True)

    gather(0)
    gather(1)
    pl.semaphore_wait(barrier, len(greeted))

    def migrants(d):
        return pltpu.make_async_remote_copy(
            src_ref=leaving.at[d],
            dst_ref=got_ref.at[d],
            send_sem=send_m.at[d],
            recv_sem=recv_m.at[d],
            device_id=ends[d][2],
            device_id_type=MESH,
        )

    held[0] = peak_ref[...]
    stages = ((along, heap_a, send_a, recv_a), (across, heap_b, send_b, recv_b), (depth, heap_c, send_c, recv_c))
    ready = ((0, 1, 2), (3,), ())
    for step, (peers, heap, send, recv) in enumerate(stages):
        copies = [
            pltpu.make_async_remote_copy(
                src_ref=held.at[step],
                dst_ref=heap.at[o],
                send_sem=send.at[o],
                recv_sem=recv.at[o],
                device_id=peer,
                device_id_type=MESH,
            )
            for o, peer in enumerate(peers)
        ]
        for copy in copies:
            copy.start()
        for d in ready[step]:
            if d > 1:
                gather(d)

            @pl.when(ends[d][0])
            def _():
                migrants(d).start()

        top = held[step]
        for o, copy in enumerate(copies):
            copy.wait()
            top = jnp.maximum(top, heap[o])
        held[step + 1] = top
    top_ref[...] = held[len(stages)]

    for d in range(4):

        @pl.when(ends[d][0])
        def _():
            migrants(d).wait_send()

        @pl.when(ends[d][1])
        def _():
            migrants(d).wait_recv()

        @pl.when(jnp.logical_not(ends[d][1]))
        def _():
            got_ref[d] = jnp.zeros(got_ref.shape[1:], jnp.float32)


def exchange(groups, counts, slots, base, moved, peak):
    inner, outer, near, far = groups
    kinds = base.shape[0] + moved.shape[0]
    cells = base.shape[1] * base.shape[2]
    width = slots.shape[1]
    dma = pltpu.SemaphoreType.DMA
    sems = []
    for peers in (inner - 1, near - 1, outer * far - 1, 4):
        sems += [dma((peers,)), dma((peers,))]
    return pl.pallas_call(
        functools.partial(exchange_kernel, groups),
        out_shape=(
            jax.ShapeDtypeStruct((4, kinds, width), jnp.float32),
            jax.ShapeDtypeStruct((SUB, LANES), jnp.float32),
        ),
        in_specs=[pl.BlockSpec(memory_space=pltpu.SMEM)] + [pl.BlockSpec(memory_space=pltpu.VMEM)] * 4,
        out_specs=(pl.BlockSpec(memory_space=pltpu.VMEM),) * 2,
        scratch_shapes=[
            pltpu.VMEM((kinds * cells, 2 * LANES), jnp.bfloat16),
            pltpu.VMEM((kinds * cells, TILE), jnp.float32),
            pltpu.VMEM((4, kinds, width), jnp.float32),
            pltpu.VMEM((4, SUB, LANES), jnp.float32),
            pltpu.VMEM((inner - 1, SUB, LANES), jnp.float32),
            pltpu.VMEM((near - 1, SUB, LANES), jnp.float32),
            pltpu.VMEM((outer * far - 1, SUB, LANES), jnp.float32),
        ]
        + sems,
        compiler_params=pltpu.CompilerParams(collective_id=0, has_side_effects=True),
    )(counts, slots, base, moved, peak)


def advance_kernel(top_ref, base_ref, moved_ref, got_ref, state_ref, arrivals_ref):
    peak_acc = jnp.sqrt(jnp.max(top_ref[0:4], axis=(0, 1), keepdims=True))
    peak_speed = jnp.sqrt(jnp.max(top_ref[4:8], axis=(0, 1), keepdims=True))
    step = 0.25 * smooth / (sound_speed + peak_speed + jnp.sqrt(smooth * peak_acc))
    for c in range(2):
        speed = base_ref[2 + c] + step * moved_ref[c]
        state_ref[2 + c] = speed
        state_ref[c] = base_ref[c] + step * speed
        state_ref[5 + c] = moved_ref[c]
    state_ref[4] = base_ref[4] + step * moved_ref[2]
    for d in range(4):
        for c in range(2):
            push = got_ref[d, 6 + c : 7 + c]
            speed = got_ref[d, 2 + c : 3 + c] + step * push
            arrivals_ref[0, 0, d, 2 + c : 3 + c] = speed
            arrivals_ref[0, 0, d, c : c + 1] = got_ref[d, c : c + 1] + step * speed
            arrivals_ref[0, 0, d, 6 + c : 7 + c] = push
        arrivals_ref[0, 0, d, 4:5] = got_ref[d, 4:5] + step * got_ref[d, 8:9]
        arrivals_ref[0, 0, d, 5:6] = got_ref[d, 5:6]


def advance(top, base, moved, got):
    return pl.pallas_call(
        advance_kernel,
        out_shape=(
            jax.ShapeDtypeStruct((7,) + base.shape[1:], jnp.float32),
            jax.ShapeDtypeStruct((1, 1, 4, 8, got.shape[2]), jnp.float32),
        ),
        in_specs=[pl.BlockSpec(memory_space=pltpu.VMEM)] * 4,
        out_specs=(pl.BlockSpec(memory_space=pltpu.VMEM),) * 2,
    )(top, base, moved, got)


def body(
    groups, positions, velocity, density, particle_mass, cell_count, wind_seed, wind_table, migrant_slot, migrant_count
):
    inner, outer, near, far = groups
    cells, base, live = halo(
        inner * outer, near * far, cell_count, positions, velocity, density, particle_mass
    )
    counts = jnp.sum(cells[:, :, 7, :], axis=2).astype(jnp.int32)
    moved, peak = all_forces(counts, wind_table, cells, wind_seed, live, base)
    got, top = exchange(groups, migrant_count[0, 0], migrant_slot[0, 0], base, moved, peak)
    return advance(top, base, moved, got)


def solution(mesh):
    shores, crosses = mesh.shape["shore"], mesh.shape["cross"]
    groups = (8, shores // 8, 8, crosses // 8)
    lined = P("shore", "cross", None)
    return jax.shard_map(
        functools.partial(body, groups),
        mesh=mesh,
        in_specs=(
            P(None, "shore", "cross", None),
            P(None, "shore", "cross", None),
            lined,
            lined,
            P("shore", "cross"),
            lined,
            P(),
            P("shore", "cross", None, None),
            lined,
        ),
        out_specs=(P(None, "shore", "cross", None), P("shore", "cross", None, None, None)),
        check_vma=False,
    )
```

```python
import functools

import jax
import jax.numpy as jnp
from jax import lax
from jax.experimental import pallas as pl
from jax.experimental.pallas import tpu as pltpu
from jax.sharding import PartitionSpec as P

MESH = pl.DeviceIdType.MESH
SUB, LANES = 8, 128
GROUP = 2
FIELDS = 7
TILE = 256
TINY = 1e-30

sound_speed = 10.0
smooth = 0.5
viscous = 0.1
kernel_norm = 7.0 / (4.0 * 3.141592653589793 * smooth * smooth)
grad_coef = -5.0 * kernel_norm / (smooth * smooth)


def pressure_ratio(density):
    cube = density * density * density
    seventh = cube * cube * density
    pressure = sound_speed * sound_speed / 7.0 * (seventh - 1.0)
    return pressure / (density * density)


def halo_kernel(
    shores, crosses, count_ref, positions_ref, velocity_ref, density_ref, mass_ref, cells_ref, base_ref, speed_ref, send, recv
):
    shore, cross = lax.axis_index("shore"), lax.axis_index("cross")
    rows, cols = density_ref.shape[:2]
    steps = [(dx, dy) for dx in (-1, 0, 1) for dy in (-1, 0, 1) if dx or dy]
    barrier = pltpu.get_barrier_semaphore()
    for dx, dy in steps:
        peer = (lax.rem(shore + dx + shores, shores), lax.rem(cross + dy + crosses, crosses))
        pl.semaphore_signal(barrier, inc=1, device_id=peer, device_id_type=MESH)

    which = lax.broadcasted_iota(jnp.int32, (cols, LANES), 0)
    slot = lax.broadcasted_iota(jnp.int32, (cols, LANES), 1)

    def pack(row, fastest):
        filled = jnp.full((cols, LANES), count_ref[row, 0], jnp.int32)
        for col in range(1, cols):
            filled = jnp.where(which == col, count_ref[row, col], filled)
        live = jnp.where(slot < filled, 1.0, 0.0)
        x, y, u, v = positions_ref[0, row], positions_ref[1, row], velocity_ref[0, row], velocity_ref[1, row]
        dense = density_ref[row]
        mass = mass_ref[row] * live
        fields = (x, y, u, v, dense, pressure_ratio(dense), grad_coef * mass, live)
        for f, value in enumerate(fields):
            cells_ref[row + 1, 1 : cols + 1, f, :] = value
        for f, value in enumerate((x * live, y * live, u * live, v * live, dense * live, mass)):
            base_ref[f, row] = value
        return jnp.maximum(fastest, (u * u + v * v) * live)

    fastest = lax.fori_loop(0, rows, pack, jnp.zeros((cols, LANES), jnp.float32))
    speed_ref[...] = jnp.full((SUB, LANES), jnp.max(fastest), jnp.float32)

    pl.semaphore_wait(barrier, len(steps))

    def edge(step, count):
        return pl.ds(1, count) if step == 0 else pl.ds(1 if step < 0 else count, 1)

    def rim(step, count):
        return pl.ds(1, count) if step == 0 else pl.ds(count + 1 if step < 0 else 0, 1)

    def inside(dx, dy):
        found = True
        for at, step, ends in ((shore, dx, shores), (cross, dy, crosses)):
            if step:
                found = jnp.logical_and(found, at < ends - 1 if step > 0 else at > 0)
        return found

    def copy(k):
        dx, dy = steps[k]
        return pltpu.make_async_remote_copy(
            src_ref=cells_ref.at[edge(dx, rows), edge(dy, cols)],
            dst_ref=cells_ref.at[rim(dx, rows), rim(dy, cols)],
            send_sem=send.at[k],
            recv_sem=recv.at[k],
            device_id=(shore + dx, cross + dy),
            device_id_type=MESH,
        )

    for k, (dx, dy) in enumerate(steps):

        @pl.when(inside(dx, dy))
        def _():
            copy(k).start()

    for k, (dx, dy) in enumerate(steps):

        @pl.when(jnp.logical_not(inside(-dx, -dy)))
        def _():
            at = (rim(dx, rows), rim(dy, cols))
            cells_ref[at] = jnp.zeros((at[0].size, at[1].size, SUB, LANES), jnp.float32)

    for k, (dx, dy) in enumerate(steps):

        @pl.when(inside(dx, dy))
        def _():
            copy(k).wait_send()

        @pl.when(inside(-dx, -dy))
        def _():
            copy(k).wait_recv()


def halo(shores, crosses, cell_count, positions, velocity, density, particle_mass):
    rows, cols = density.shape[:2]
    vmem = pl.BlockSpec(memory_space=pltpu.VMEM)
    return pl.pallas_call(
        functools.partial(halo_kernel, shores, crosses),
        out_shape=(
            jax.ShapeDtypeStruct((rows + 2, cols + 2, SUB, LANES), jnp.float32),
            jax.ShapeDtypeStruct((6, rows, cols, LANES), jnp.float32),
            jax.ShapeDtypeStruct((SUB, LANES), jnp.float32),
        ),
        in_specs=[pl.BlockSpec(memory_space=pltpu.SMEM)] + [vmem] * 4,
        out_specs=(vmem,) * 3,
        scratch_shapes=[pltpu.SemaphoreType.DMA((8,)), pltpu.SemaphoreType.DMA((8,))],
        compiler_params=pltpu.CompilerParams(collective_id=1, has_side_effects=True),
    )(cell_count, positions, velocity, density, particle_mass)


def halves(exact, parts):
    got = []
    for _ in range(parts):
        got.append(exact.astype(jnp.bfloat16))
        exact = exact - got[-1].astype(jnp.float32)
    return got


def force_kernel(
    table_ref, cells_ref, pick_ref, seed_ref, out_ref, peak_ref, placed, wide, sums, returned, counts
):
    height, width = cells_ref.shape[:2]
    rows, cols = height - 2, width - 2
    field = lax.broadcasted_iota(jnp.int32, (SUB, LANES), 0)

    @pl.loop(0, height)
    def _(row):
        for col in range(width):
            shift = jnp.where(field == 0, row.astype(jnp.float32), jnp.where(field == 1, float(col), 0.0))
            placed[row, col] = cells_ref[row, col] + shift

    @pl.loop(0, rows)
    def _(row):
        for col in range(cols):
            for c in range(3):
                sums[row, col, c] = jnp.zeros((SUB, LANES), jnp.float32)

    def widen(row, col):
        counts[row, col] = jnp.sum(cells_ref[row, col, 7:8, :]).astype(jnp.int32)
        split = jnp.concatenate([x.astype(jnp.float32) for x in halves(placed[row, col], 3)], axis=0)
        wide[col] = lax.dot_general(
            jnp.transpose(split).astype(jnp.bfloat16),
            pick_ref[...],
            (((1,), (0,)), ((), ())),
            preferred_element_type=jnp.float32,
        )

    def gather_back(row, col):
        for k in range(3):
            turned = jnp.transpose(returned[col, k])
            total = turned[0:SUB]
            for v in range(1, LANES // SUB):
                total = total + turned[v * SUB : (v + 1) * SUB]
            sums[row - 1, col, k] += total if k == 2 else -total

    def turn(row, gathered):
        for col in range(width):
            widen(row + 1, col)
            if col < gathered:
                gather_back(row, col)

    def loop_over(row, col):
        count = lax.div(counts[row, col] + (SUB * GROUP - 1), SUB * GROUP)

        def loaded(part):
            near = []
            for g in range(GROUP):
                at = pl.ds(pl.multiple_of((part * GROUP + g) * SUB, SUB), SUB)
                near.append(tuple(wide[col, at, f * LANES : (f + 1) * LANES] for f in range(FIELDS)))
            return near

        return count, loaded

    def shared(own, near):
        xi, yi, ui, vi, di, pi = own
        xj, yj, uj, vj, dj, pj = near
        ox = xi - xj
        oy = yi - yj
        d2 = ox * ox + oy * oy
        near_d2 = jnp.clip(d2, TINY, 1.0)
        f = 1.0 - near_d2 * lax.rsqrt(near_d2)
        f3 = f * f * f
        a = (ui - uj) * ox + (vi - vj) * oy
        q = (d2 + 0.01 * smooth * smooth) * (di + dj)
        return ox, oy, f3, a, (pi + pj) - jnp.minimum(a, 0.0) * pl.reciprocal(q)

    def row_of(row, col, f):
        return jnp.broadcast_to(placed[row, col, f : f + 1, :], (SUB, LANES))

    def plus(total, terms):
        return terms if total is None else tuple(t + x for t, x in zip(total, terms))

    def one_way(row, col, step, near):
        own = (row + step[0], col + step[1])
        fields = [row_of(own[0], own[1], f) for f in range(6)]
        mass = row_of(own[0], own[1], 6)
        total = None
        for there in near:
            ox, oy, f3, a, c = shared(fields, there[:6])
            w = mass * there[6] * f3
            c = w * c
            total = plus(total, (c * ox, c * oy, w * a))
        for k in range(3):
            sums[own[0] - 1, own[1] - 1, k] += total[k]

    def both_ways(row, col, step, near, back):
        own = (row + step[0], col + step[1])
        fields = [row_of(own[0], own[1], f) for f in range(6)]
        mass = row_of(own[0], own[1], 6)
        total = None
        for g, there in enumerate(near):
            ox, oy, f3, a, c = shared(fields, there[:6])
            w = mass * there[6] * f3
            c = w * c
            terms = (c * ox, c * oy, w * a)
            total = plus(total, terms)
            back[g] = plus(back[g], terms)
        for k in range(3):
            sums[own[0] - 1, own[1] - 1, k] += total[k]

    def outer_cell(row, col, steps):
        count, loaded = loop_over(row, col)

        @pl.loop(0, count)
        def _(part):
            near = loaded(part)
            for step in steps:
                one_way(row, col, step, near)

    def inner_cell(row, col, steps):
        count, loaded = loop_over(row, col)

        @pl.loop(0, count)
        def _(part):
            near = loaded(part)
            back = [None] * GROUP
            one_way(row, col, (0, 0), near)
            for step in steps:
                both_ways(row, col, step, near, back)
            for g in range(GROUP):
                if back[g] is not None:
                    at = pl.ds(pl.multiple_of((part * GROUP + g) * SUB, SUB), SUB)
                    for k in range(3):
                        returned[col - 1, k, at, :] = back[g][k]

    def outer_row(row, step):
        outer_cell(row, 0, ((step, 1),))
        outer_cell(row, 1, ((step, 0), (step, 1)))

        @pl.loop(2, width - 2)
        def _(col):
            outer_cell(row, col, ((step, -1), (step, 0), (step, 1)))

        outer_cell(row, width - 2, ((step, -1), (step, 0)))
        outer_cell(row, width - 1, ((step, -1),))

    def inner_row(row, drs, last):
        outer_cell(row, 0, tuple((dr, 1) for dr in drs))
        outer_cell(row, width - 1, tuple((dr, -1) for dr in drs))
        down = () if last else ((1, -1), (1, 0), (1, 1))
        inner_cell(row, 1, ((0, 1),) + down[1:])

        @pl.loop(2, width - 2)
        def _(col):
            inner_cell(row, col, ((0, 1),) + down)

        inner_cell(row, width - 2, down[:2])
        turn(row, cols - 1 if last else cols)

    @pl.loop(0, cols)
    def _(col):
        for k in range(3):
            returned[col, k] = jnp.zeros((LANES, LANES), jnp.float32)

    for col in range(width):
        widen(0, col)
    outer_row(0, 1)
    for col in range(width):
        widen(1, col)
    inner_row(1, (0, 1), False)

    @pl.loop(2, height - 2)
    def _(row):
        inner_row(row, (-1, 0, 1), False)

    inner_row(height - 2, (-1, 0), True)
    outer_row(height - 1, -1)

    def finish(row, peak):
        live = placed[row + 1, 1 : cols + 1, 7, :]
        mass = placed[row + 1, 1 : cols + 1, 6, :]
        per_mass = jnp.where(live > 0.0, 1.0 / mass, 0.0)
        seed = seed_ref[row]
        got = []
        for c in range(3):
            ends = [jnp.sum(sums[row, col, c], axis=0, keepdims=True) for col in range(cols)]
            got.append(jnp.concatenate(ends, axis=0) * per_mass)
        acc = []
        for c in range(2):
            wind = jnp.full(seed.shape, table_ref[c, 0], jnp.float32)
            for level in range(1, table_ref.shape[1]):
                wind = jnp.where(seed == level, table_ref[c, level], wind)
            acc.append((wind - got[c]) * live)
            out_ref[c, row] = acc[c]
        out_ref[2, row] = got[2] * live
        return jnp.maximum(peak, acc[0] * acc[0] + acc[1] * acc[1])

    peak = lax.fori_loop(0, rows, finish, jnp.zeros((cols, LANES), jnp.float32))
    peak_ref[...] = jnp.full((SUB, LANES), jnp.max(peak), jnp.float32)


def all_forces(table, cells, seed):
    height, width = cells.shape[:2]
    rows, cols = height - 2, width - 2
    which = lax.broadcasted_iota(jnp.int32, (24, FIELDS * LANES), 0) % 8
    pick = (which == lax.broadcasted_iota(jnp.int32, (24, FIELDS * LANES), 1) // LANES).astype(jnp.bfloat16)
    return pl.pallas_call(
        force_kernel,
        out_shape=(
            jax.ShapeDtypeStruct((3, rows, cols, LANES), jnp.float32),
            jax.ShapeDtypeStruct((SUB, LANES), jnp.float32),
        ),
        in_specs=[pl.BlockSpec(memory_space=pltpu.SMEM)] + [pl.BlockSpec(memory_space=pltpu.VMEM)] * 3,
        out_specs=(pl.BlockSpec(memory_space=pltpu.VMEM),) * 2,
        scratch_shapes=[
            pltpu.VMEM((height, width, SUB, LANES), jnp.float32),
            pltpu.VMEM((width, LANES, FIELDS * LANES), jnp.float32),
            pltpu.VMEM((rows, cols, 3, SUB, LANES), jnp.float32),
            pltpu.VMEM((cols, 3, LANES, LANES), jnp.float32),
            pltpu.SMEM((height, width), jnp.int32),
        ],
        compiler_params=pltpu.CompilerParams(vmem_limit_bytes=32 << 20),
    )(table, cells, pick, seed)


def exchange_kernel(
    groups, counts_ref, slots_ref, base_ref, moved_ref, peak_ref, speed_ref, got_ref, top_ref,
    split, found, leaving, held, heap_a, heap_b, heap_c, send_a, recv_a, send_b, recv_b, send_c, recv_c, send_m, recv_m,
):
    inner, outer, near, far = groups
    shore, cross = lax.axis_index("shore"), lax.axis_index("cross")
    shores, crosses = inner * outer, near * far
    s_out, s_in = lax.div(shore, inner), lax.rem(shore, inner)
    c_out, c_in = lax.div(cross, near), lax.rem(cross, near)

    along = [
        (s_out * inner + lax.rem(s_in + o, inner), cross) for o in range(1, inner)
    ]
    across = [(shore, c_out * near + lax.rem(c_in + o, near)) for o in range(1, near)]
    depth = []
    for o in range(1, outer * far):
        spot = lax.rem(s_out * far + c_out + o, outer * far)
        depth.append((lax.div(spot, far) * inner + s_in, lax.rem(spot, far) * near + c_in))
    ends = [
        (shore < shores - 1, shore > 0, (shore + 1, cross)),
        (shore > 0, shore < shores - 1, (shore - 1, cross)),
        (cross < crosses - 1, cross > 0, (shore, cross + 1)),
        (cross > 0, cross < crosses - 1, (shore, cross - 1)),
    ]

    barrier = pltpu.get_barrier_semaphore()
    beside = [
        (lax.rem(shore + 1, shores), cross),
        (lax.rem(shore + shores - 1, shores), cross),
        (shore, lax.rem(cross + 1, crosses)),
        (shore, lax.rem(cross + crosses - 1, crosses)),
    ]
    greeted = along + across + depth + beside
    for peer in greeted:
        pl.semaphore_signal(barrier, inc=1, device_id=peer, device_id_type=MESH)

    kinds = base_ref.shape[0] + moved_ref.shape[0]
    cells = base_ref.shape[1] * base_ref.shape[2]
    for f in range(kinds):
        source = base_ref[f] if f < base_ref.shape[0] else moved_ref[f - base_ref.shape[0]]
        high, low = halves(source.reshape(cells, LANES), 2)
        split[f * cells : (f + 1) * cells, 0:LANES] = high
        split[f * cells : (f + 1) * cells, LANES : 2 * LANES] = low

    width = slots_ref.shape[1]
    rank = lax.broadcasted_iota(jnp.int32, (LANES, TILE), 0)

    def gather(d):
        @pl.loop(0, width // TILE)
        def _(t):
            at = pl.ds(pl.multiple_of(t * TILE, TILE), TILE)
            slot = slots_ref[d : d + 1, at]
            lane = jnp.where(rank == (slot & (LANES - 1)), 1.0, 0.0)
            lanes = jnp.concatenate([lane, lane], axis=0).astype(jnp.bfloat16)
            found[...] = jnp.dot(split[...], lanes, preferred_element_type=jnp.float32)
            order = lax.broadcasted_iota(jnp.int32, (1, TILE), 1) + t * TILE
            cell = jnp.where(order < counts_ref[d], lax.shift_right_logical(slot, 7), -1)
            keep = rank == cell
            for f in range(kinds):
                mine = found[f * cells : (f + 1) * cells, :]
                leaving[d, f : f + 1, at] = jnp.sum(jnp.where(keep, mine, 0.0), axis=0, keepdims=True)

    gather(0)
    gather(1)
    pl.semaphore_wait(barrier, len(greeted))

    def migrants(d):
        return pltpu.make_async_remote_copy(
            src_ref=leaving.at[d],
            dst_ref=got_ref.at[d],
            send_sem=send_m.at[d],
            recv_sem=recv_m.at[d],
            device_id=ends[d][2],
            device_id_type=MESH,
        )

    field = lax.broadcasted_iota(jnp.int32, (SUB, LANES), 0)
    held[0] = jnp.where(field < 4, peak_ref[...], speed_ref[...])
    stages = ((along, heap_a, send_a, recv_a), (across, heap_b, send_b, recv_b), (depth, heap_c, send_c, recv_c))
    ready = ((0, 1, 2), (3,), ())
    for step, (peers, heap, send, recv) in enumerate(stages):
        copies = [
            pltpu.make_async_remote_copy(
                src_ref=held.at[step],
                dst_ref=heap.at[o],
                send_sem=send.at[o],
                recv_sem=recv.at[o],
                device_id=peer,
                device_id_type=MESH,
            )
            for o, peer in enumerate(peers)
        ]
        for copy in copies:
            copy.start()
        for d in ready[step]:
            if d > 1:
                gather(d)

            @pl.when(ends[d][0])
            def _():
                migrants(d).start()

        top = held[step]
        for o, copy in enumerate(copies):
            copy.wait()
            top = jnp.maximum(top, heap[o])
        held[step + 1] = top
    top_ref[...] = held[len(stages)]

    for d in range(4):

        @pl.when(ends[d][0])
        def _():
            migrants(d).wait_send()

        @pl.when(ends[d][1])
        def _():
            migrants(d).wait_recv()

        @pl.when(jnp.logical_not(ends[d][1]))
        def _():
            got_ref[d] = jnp.zeros(got_ref.shape[1:], jnp.float32)


def exchange(groups, counts, slots, base, moved, peak, speed):
    inner, outer, near, far = groups
    kinds = base.shape[0] + moved.shape[0]
    cells = base.shape[1] * base.shape[2]
    width = slots.shape[1]
    dma = pltpu.SemaphoreType.DMA
    sems = []
    for peers in (inner - 1, near - 1, outer * far - 1, 4):
        sems += [dma((peers,)), dma((peers,))]
    return pl.pallas_call(
        functools.partial(exchange_kernel, groups),
        out_shape=(
            jax.ShapeDtypeStruct((4, kinds, width), jnp.float32),
            jax.ShapeDtypeStruct((SUB, LANES), jnp.float32),
        ),
        in_specs=[pl.BlockSpec(memory_space=pltpu.SMEM)] + [pl.BlockSpec(memory_space=pltpu.VMEM)] * 5,
        out_specs=(pl.BlockSpec(memory_space=pltpu.VMEM),) * 2,
        scratch_shapes=[
            pltpu.VMEM((kinds * cells, 2 * LANES), jnp.bfloat16),
            pltpu.VMEM((kinds * cells, TILE), jnp.float32),
            pltpu.VMEM((4, kinds, width), jnp.float32),
            pltpu.VMEM((4, SUB, LANES), jnp.float32),
            pltpu.VMEM((inner - 1, SUB, LANES), jnp.float32),
            pltpu.VMEM((near - 1, SUB, LANES), jnp.float32),
            pltpu.VMEM((outer * far - 1, SUB, LANES), jnp.float32),
        ]
        + sems,
        compiler_params=pltpu.CompilerParams(collective_id=0, has_side_effects=True),
    )(counts, slots, base, moved, peak, speed)


def advance_kernel(top_ref, base_ref, moved_ref, got_ref, state_ref, arrivals_ref):
    peak_acc = jnp.sqrt(jnp.max(top_ref[0:4], axis=(0, 1), keepdims=True))
    peak_speed = jnp.sqrt(jnp.max(top_ref[4:8], axis=(0, 1), keepdims=True))
    step = 0.25 * smooth / (sound_speed + peak_speed + jnp.sqrt(smooth * peak_acc))
    for c in range(2):
        speed = base_ref[2 + c] + step * moved_ref[c]
        state_ref[2 + c] = speed
        state_ref[c] = base_ref[c] + step * speed
        state_ref[5 + c] = moved_ref[c]
    state_ref[4] = base_ref[4] + step * moved_ref[2]
    for d in range(4):
        for c in range(2):
            push = got_ref[d, 6 + c : 7 + c]
            speed = got_ref[d, 2 + c : 3 + c] + step * push
            arrivals_ref[0, 0, d, 2 + c : 3 + c] = speed
            arrivals_ref[0, 0, d, c : c + 1] = got_ref[d, c : c + 1] + step * speed
            arrivals_ref[0, 0, d, 6 + c : 7 + c] = push
        arrivals_ref[0, 0, d, 4:5] = got_ref[d, 4:5] + step * got_ref[d, 8:9]
        arrivals_ref[0, 0, d, 5:6] = got_ref[d, 5:6]


def advance(top, base, moved, got):
    return pl.pallas_call(
        advance_kernel,
        out_shape=(
            jax.ShapeDtypeStruct((7,) + base.shape[1:], jnp.float32),
            jax.ShapeDtypeStruct((1, 1, 4, 8, got.shape[2]), jnp.float32),
        ),
        in_specs=[pl.BlockSpec(memory_space=pltpu.VMEM)] * 4,
        out_specs=(pl.BlockSpec(memory_space=pltpu.VMEM),) * 2,
    )(top, base, moved, got)


def body(
    groups, positions, velocity, density, particle_mass, cell_count, wind_seed, wind_table, migrant_slot, migrant_count
):
    inner, outer, near, far = groups
    cells, base, speed = halo(
        inner * outer, near * far, cell_count, positions, velocity, density, particle_mass
    )
    moved, peak = all_forces(wind_table, cells, wind_seed)
    got, top = exchange(groups, migrant_count[0, 0], migrant_slot[0, 0], base, moved, peak, speed)
    return advance(top, base, moved, got)


def solution(mesh):
    shores, crosses = mesh.shape["shore"], mesh.shape["cross"]
    groups = (8, shores // 8, 8, crosses // 8)
    lined = P("shore", "cross", None)
    return jax.shard_map(
        functools.partial(body, groups),
        mesh=mesh,
        in_specs=(
            P(None, "shore", "cross", None),
            P(None, "shore", "cross", None),
            lined,
            lined,
            P("shore", "cross"),
            lined,
            P(),
            P("shore", "cross", None, None),
            lined,
        ),
        out_specs=(P(None, "shore", "cross", None), P("shore", "cross", None, None, None)),
        check_vma=False,
    )
```

```python
import functools

import jax
import jax.numpy as jnp
from jax import lax
from jax.experimental import pallas as pl
from jax.experimental.pallas import tpu as pltpu
from jax.sharding import PartitionSpec as P

MESH = pl.DeviceIdType.MESH
SUB, LANES = 8, 128
GROUP = 2
FIELDS = 7
TILE = 256
TINY = 1e-30

sound_speed = 10.0
smooth = 0.5
viscous = 0.1
kernel_norm = 7.0 / (4.0 * 3.141592653589793 * smooth * smooth)
grad_coef = -5.0 * kernel_norm / (smooth * smooth)


def pressure_ratio(density):
    cube = density * density * density
    seventh = cube * cube * density
    pressure = sound_speed * sound_speed / 7.0 * (seventh - 1.0)
    return pressure / (density * density)


def halo_kernel(
    shores, crosses, count_ref, positions_ref, velocity_ref, density_ref, mass_ref, cells_ref, base_ref, speed_ref, send, recv
):
    shore, cross = lax.axis_index("shore"), lax.axis_index("cross")
    rows, cols = density_ref.shape[:2]
    steps = [(dx, dy) for dx in (-1, 0, 1) for dy in (-1, 0, 1) if dx or dy]
    barrier = pltpu.get_barrier_semaphore()
    for dx, dy in steps:
        peer = (lax.rem(shore + dx + shores, shores), lax.rem(cross + dy + crosses, crosses))
        pl.semaphore_signal(barrier, inc=1, device_id=peer, device_id_type=MESH)

    which = lax.broadcasted_iota(jnp.int32, (cols, LANES), 0)
    slot = lax.broadcasted_iota(jnp.int32, (cols, LANES), 1)

    def pack(row, fastest):
        filled = jnp.full((cols, LANES), count_ref[0, row], jnp.int32)
        for col in range(1, cols):
            filled = jnp.where(which == col, count_ref[col, row], filled)
        live = jnp.where(slot < filled, 1.0, 0.0)
        x, y, u, v = positions_ref[0, row], positions_ref[1, row], velocity_ref[0, row], velocity_ref[1, row]
        dense = density_ref[row]
        mass = mass_ref[row] * live
        fields = (x, y, u, v, dense, pressure_ratio(dense), grad_coef * mass, live)
        for f, value in enumerate(fields):
            cells_ref[row + 1, 1 : cols + 1, f, :] = value
        for f, value in enumerate((x * live, y * live, u * live, v * live, dense * live, mass)):
            base_ref[f, row] = value
        return jnp.maximum(fastest, (u * u + v * v) * live)

    fastest = lax.fori_loop(0, rows, pack, jnp.zeros((cols, LANES), jnp.float32))
    speed_ref[...] = jnp.full((SUB, LANES), jnp.max(fastest), jnp.float32)

    pl.semaphore_wait(barrier, len(steps))

    def edge(step, count):
        return pl.ds(1, count) if step == 0 else pl.ds(1 if step < 0 else count, 1)

    def rim(step, count):
        return pl.ds(1, count) if step == 0 else pl.ds(count + 1 if step < 0 else 0, 1)

    def inside(dx, dy):
        found = True
        for at, step, ends in ((shore, dx, shores), (cross, dy, crosses)):
            if step:
                found = jnp.logical_and(found, at < ends - 1 if step > 0 else at > 0)
        return found

    def copy(k):
        dx, dy = steps[k]
        return pltpu.make_async_remote_copy(
            src_ref=cells_ref.at[edge(dx, rows), edge(dy, cols)],
            dst_ref=cells_ref.at[rim(dx, rows), rim(dy, cols)],
            send_sem=send.at[k],
            recv_sem=recv.at[k],
            device_id=(shore + dx, cross + dy),
            device_id_type=MESH,
        )

    for k, (dx, dy) in enumerate(steps):

        @pl.when(inside(dx, dy))
        def _():
            copy(k).start()

    for k, (dx, dy) in enumerate(steps):

        @pl.when(jnp.logical_not(inside(-dx, -dy)))
        def _():
            at = (rim(dx, rows), rim(dy, cols))
            cells_ref[at] = jnp.zeros((at[0].size, at[1].size, SUB, LANES), jnp.float32)

    for k, (dx, dy) in enumerate(steps):

        @pl.when(inside(dx, dy))
        def _():
            copy(k).wait_send()

        @pl.when(inside(-dx, -dy))
        def _():
            copy(k).wait_recv()


def halo(shores, crosses, cell_count, positions, velocity, density, particle_mass):
    rows, cols = density.shape[:2]
    vmem = pl.BlockSpec(memory_space=pltpu.VMEM)
    return pl.pallas_call(
        functools.partial(halo_kernel, shores, crosses),
        out_shape=(
            jax.ShapeDtypeStruct((rows + 2, cols + 2, SUB, LANES), jnp.float32),
            jax.ShapeDtypeStruct((6, rows, cols, LANES), jnp.float32),
            jax.ShapeDtypeStruct((SUB, LANES), jnp.float32),
        ),
        in_specs=[pl.BlockSpec(memory_space=pltpu.SMEM)] + [vmem] * 4,
        out_specs=(vmem,) * 3,
        scratch_shapes=[pltpu.SemaphoreType.DMA((8,)), pltpu.SemaphoreType.DMA((8,))],
        compiler_params=pltpu.CompilerParams(collective_id=1, has_side_effects=True),
    )(cell_count, positions, velocity, density, particle_mass)


def halves(exact, parts):
    got = []
    for _ in range(parts):
        got.append(exact.astype(jnp.bfloat16))
        exact = exact - got[-1].astype(jnp.float32)
    return got


def force_kernel(
    table_ref, cells_ref, pick_ref, seed_ref, out_ref, peak_ref, placed, wide, sums, returned, counts
):
    height, width = cells_ref.shape[:2]
    rows, cols = height - 2, width - 2
    field = lax.broadcasted_iota(jnp.int32, (SUB, LANES), 0)

    @pl.loop(0, height)
    def _(row):
        for col in range(width):
            shift = jnp.where(field == 0, row.astype(jnp.float32), jnp.where(field == 1, float(col), 0.0))
            placed[row, col] = cells_ref[row, col] + shift

    @pl.loop(0, rows)
    def _(row):
        for col in range(cols):
            for c in range(3):
                sums[row, col, c] = jnp.zeros((SUB, LANES), jnp.float32)

    def widen(row, col):
        counts[row, col] = jnp.sum(cells_ref[row, col, 7:8, :]).astype(jnp.int32)
        split = jnp.concatenate([x.astype(jnp.float32) for x in halves(placed[row, col], 3)], axis=0)
        wide[col] = lax.dot_general(
            jnp.transpose(split).astype(jnp.bfloat16),
            pick_ref[...],
            (((1,), (0,)), ((), ())),
            preferred_element_type=jnp.float32,
        )

    def gather_back(row, col):
        for k in range(3):
            turned = jnp.transpose(returned[col, k])
            total = turned[0:SUB]
            for v in range(1, LANES // SUB):
                total = total + turned[v * SUB : (v + 1) * SUB]
            sums[row - 1, col, k] += total if k == 2 else -total

    def loop_over(row, col):
        count = lax.div(counts[row, col] + (SUB * GROUP - 1), SUB * GROUP)

        def loaded(part):
            near = []
            for g in range(GROUP):
                at = pl.ds(pl.multiple_of((part * GROUP + g) * SUB, SUB), SUB)
                near.append(tuple(wide[col, at, f * LANES : (f + 1) * LANES] for f in range(FIELDS)))
            return near

        return count, loaded

    def shared(own, near):
        xi, yi, ui, vi, di, pi = own
        xj, yj, uj, vj, dj, pj = near
        ox = xi - xj
        oy = yi - yj
        d2 = ox * ox + oy * oy
        near_d2 = jnp.clip(d2, TINY, 1.0)
        f = 1.0 - near_d2 * lax.rsqrt(near_d2)
        f3 = f * f * f
        a = (ui - uj) * ox + (vi - vj) * oy
        q = (d2 + 0.01 * smooth * smooth) * (di + dj)
        return ox, oy, f3, a, (pi + pj) - jnp.minimum(a, 0.0) * pl.reciprocal(q)

    def row_of(row, col, f):
        return jnp.broadcast_to(placed[row, col, f : f + 1, :], (SUB, LANES))

    def plus(total, terms):
        return terms if total is None else tuple(t + x for t, x in zip(total, terms))

    def one_way(row, col, step, near):
        own = (row + step[0], col + step[1])
        fields = [row_of(own[0], own[1], f) for f in range(6)]
        mass = row_of(own[0], own[1], 6)
        total = None
        for there in near:
            ox, oy, f3, a, c = shared(fields, there[:6])
            w = mass * there[6] * f3
            c = w * c
            total = plus(total, (c * ox, c * oy, w * a))
        for k in range(3):
            sums[own[0] - 1, own[1] - 1, k] += total[k]

    def both_ways(row, col, step, near, back, keep):
        own = (row + step[0], col + step[1])
        fields = [row_of(own[0], own[1], f) for f in range(6)]
        mass = row_of(own[0], own[1], 6)
        total = None
        for g, there in enumerate(near):
            ox, oy, f3, a, c = shared(fields, there[:6])
            w = mass * there[6] * f3
            c = w * c
            terms = (c * ox, c * oy, w * a)
            total = plus(total, terms)
            back[g] = plus(back[g], terms)
        if keep:
            for k in range(3):
                sums[own[0] - 1, own[1] - 1, k] += total[k]

    def one_cell(row, col, mutual, rim):
        count, loaded = loop_over(row, col)

        @pl.loop(0, count)
        def _(part):
            near = loaded(part)
            back = [None] * GROUP
            one_way(row, col, (0, 0), near)
            for step in mutual:
                both_ways(row, col, step, near, back, True)
            for step in rim:
                both_ways(row, col, step, near, back, False)
            for g in range(GROUP):
                at = pl.ds(pl.multiple_of((part * GROUP + g) * SUB, SUB), SUB)
                for k in range(3):
                    returned[col - 1, k, at, :] = back[g][k]

    def one_row(row, first, last):
        def cell(col, leftmost, rightmost):
            mutual, rim = [], []
            for step in ((-1, -1), (-1, 0), (-1, 1), (0, -1), (0, 1), (1, -1), (1, 0), (1, 1)):
                dr, dc = step
                outside = (first and dr < 0) or (last and dr > 0) or (leftmost and dc < 0) or (rightmost and dc > 0)
                if outside:
                    rim.append(step)
                elif dr > 0 or (dr == 0 and dc > 0):
                    mutual.append(step)
            one_cell(row, col, mutual, rim)

        cell(1, True, False)

        @pl.loop(2, cols)
        def _(col):
            cell(col, False, False)

        cell(cols, False, True)
        for col in range(1, cols + 1):
            if not last:
                widen(row + 1, col)
            gather_back(row, col - 1)

    @pl.loop(0, cols)
    def _(col):
        for k in range(3):
            returned[col, k] = jnp.zeros((LANES, LANES), jnp.float32)

    for col in range(1, cols + 1):
        widen(1, col)
    one_row(1, True, False)

    @pl.loop(2, rows)
    def _(row):
        one_row(row, False, False)

    one_row(rows, False, True)

    def finish(row, peak):
        live = placed[row + 1, 1 : cols + 1, 7, :]
        mass = placed[row + 1, 1 : cols + 1, 6, :]
        per_mass = jnp.where(live > 0.0, 1.0 / mass, 0.0)
        seed = seed_ref[row]
        got = []
        for c in range(3):
            ends = [jnp.sum(sums[row, col, c], axis=0, keepdims=True) for col in range(cols)]
            got.append(jnp.concatenate(ends, axis=0) * per_mass)
        acc = []
        for c in range(2):
            wind = jnp.full(seed.shape, table_ref[c, 0], jnp.float32)
            for level in range(1, table_ref.shape[1]):
                wind = jnp.where(seed == level, table_ref[c, level], wind)
            acc.append((wind - got[c]) * live)
            out_ref[c, row] = acc[c]
        out_ref[2, row] = got[2] * live
        return jnp.maximum(peak, acc[0] * acc[0] + acc[1] * acc[1])

    peak = lax.fori_loop(0, rows, finish, jnp.zeros((cols, LANES), jnp.float32))
    peak_ref[...] = jnp.full((SUB, LANES), jnp.max(peak), jnp.float32)


def all_forces(table, cells, seed):
    height, width = cells.shape[:2]
    rows, cols = height - 2, width - 2
    which = lax.broadcasted_iota(jnp.int32, (24, FIELDS * LANES), 0) % 8
    pick = (which == lax.broadcasted_iota(jnp.int32, (24, FIELDS * LANES), 1) // LANES).astype(jnp.bfloat16)
    return pl.pallas_call(
        force_kernel,
        out_shape=(
            jax.ShapeDtypeStruct((3, rows, cols, LANES), jnp.float32),
            jax.ShapeDtypeStruct((SUB, LANES), jnp.float32),
        ),
        in_specs=[pl.BlockSpec(memory_space=pltpu.SMEM)] + [pl.BlockSpec(memory_space=pltpu.VMEM)] * 3,
        out_specs=(pl.BlockSpec(memory_space=pltpu.VMEM),) * 2,
        scratch_shapes=[
            pltpu.VMEM((height, width, SUB, LANES), jnp.float32),
            pltpu.VMEM((width, LANES, FIELDS * LANES), jnp.float32),
            pltpu.VMEM((rows, cols, 3, SUB, LANES), jnp.float32),
            pltpu.VMEM((cols, 3, LANES, LANES), jnp.float32),
            pltpu.SMEM((height, width), jnp.int32),
        ],
        compiler_params=pltpu.CompilerParams(vmem_limit_bytes=32 << 20),
    )(table, cells, pick, seed)


def exchange_kernel(
    groups, counts_ref, slots_ref, base_ref, moved_ref, peak_ref, speed_ref, got_ref, top_ref,
    split, found, leaving, held, heap_a, heap_b, heap_c, send_a, recv_a, send_b, recv_b, send_c, recv_c, send_m, recv_m,
):
    inner, outer, near, far = groups
    shore, cross = lax.axis_index("shore"), lax.axis_index("cross")
    shores, crosses = inner * outer, near * far
    s_out, s_in = lax.div(shore, inner), lax.rem(shore, inner)
    c_out, c_in = lax.div(cross, near), lax.rem(cross, near)

    along = [
        (s_out * inner + lax.rem(s_in + o, inner), cross) for o in range(1, inner)
    ]
    across = [(shore, c_out * near + lax.rem(c_in + o, near)) for o in range(1, near)]
    depth = []
    for o in range(1, outer * far):
        spot = lax.rem(s_out * far + c_out + o, outer * far)
        depth.append((lax.div(spot, far) * inner + s_in, lax.rem(spot, far) * near + c_in))
    ends = [
        (shore < shores - 1, shore > 0, (shore + 1, cross)),
        (shore > 0, shore < shores - 1, (shore - 1, cross)),
        (cross < crosses - 1, cross > 0, (shore, cross + 1)),
        (cross > 0, cross < crosses - 1, (shore, cross - 1)),
    ]

    barrier = pltpu.get_barrier_semaphore()
    beside = [
        (lax.rem(shore + 1, shores), cross),
        (lax.rem(shore + shores - 1, shores), cross),
        (shore, lax.rem(cross + 1, crosses)),
        (shore, lax.rem(cross + crosses - 1, crosses)),
    ]
    greeted = along + across + depth + beside
    for peer in greeted:
        pl.semaphore_signal(barrier, inc=1, device_id=peer, device_id_type=MESH)

    kinds = base_ref.shape[0] + moved_ref.shape[0]
    cells = base_ref.shape[1] * base_ref.shape[2]
    for f in range(kinds):
        source = base_ref[f] if f < base_ref.shape[0] else moved_ref[f - base_ref.shape[0]]
        high, low = halves(source.reshape(cells, LANES), 2)
        split[f * cells : (f + 1) * cells, 0:LANES] = high
        split[f * cells : (f + 1) * cells, LANES : 2 * LANES] = low

    width = slots_ref.shape[1]
    rank = lax.broadcasted_iota(jnp.int32, (LANES, TILE), 0)

    def gather(d):
        @pl.loop(0, width // TILE)
        def _(t):
            at = pl.ds(pl.multiple_of(t * TILE, TILE), TILE)
            slot = slots_ref[d : d + 1, at]
            lane = jnp.where(rank == (slot & (LANES - 1)), 1.0, 0.0)
            lanes = jnp.concatenate([lane, lane], axis=0).astype(jnp.bfloat16)
            found[...] = jnp.dot(split[...], lanes, preferred_element_type=jnp.float32)
            order = lax.broadcasted_iota(jnp.int32, (1, TILE), 1) + t * TILE
            cell = jnp.where(order < counts_ref[d], lax.shift_right_logical(slot, 7), -1)
            keep = rank == cell
            for f in range(kinds):
                mine = found[f * cells : (f + 1) * cells, :]
                leaving[d, f : f + 1, at] = jnp.sum(jnp.where(keep, mine, 0.0), axis=0, keepdims=True)

    gather(0)
    gather(1)
    gather(2)
    pl.semaphore_wait(barrier, len(greeted))

    def migrants(d):
        return pltpu.make_async_remote_copy(
            src_ref=leaving.at[d],
            dst_ref=got_ref.at[d],
            send_sem=send_m.at[d],
            recv_sem=recv_m.at[d],
            device_id=ends[d][2],
            device_id_type=MESH,
        )

    field = lax.broadcasted_iota(jnp.int32, (SUB, LANES), 0)
    held[0] = jnp.where(field < 4, peak_ref[...], speed_ref[...])
    stages = ((along, heap_a, send_a, recv_a), (across, heap_b, send_b, recv_b), (depth, heap_c, send_c, recv_c))
    ready = ((0, 1, 2, 3), (), ())
    for step, (peers, heap, send, recv) in enumerate(stages):
        copies = [
            pltpu.make_async_remote_copy(
                src_ref=held.at[step],
                dst_ref=heap.at[o],
                send_sem=send.at[o],
                recv_sem=recv.at[o],
                device_id=peer,
                device_id_type=MESH,
            )
            for o, peer in enumerate(peers)
        ]
        for copy in copies:
            copy.start()
        for d in ready[step]:
            if d > 2:
                gather(d)

            @pl.when(ends[d][0])
            def _():
                migrants(d).start()

        top = held[step]
        for o, copy in enumerate(copies):
            copy.wait()
            top = jnp.maximum(top, heap[o])
        held[step + 1] = top
    top_ref[...] = held[len(stages)]

    for d in range(4):

        @pl.when(ends[d][0])
        def _():
            migrants(d).wait_send()

        @pl.when(ends[d][1])
        def _():
            migrants(d).wait_recv()

        @pl.when(jnp.logical_not(ends[d][1]))
        def _():
            got_ref[d] = jnp.zeros(got_ref.shape[1:], jnp.float32)


def exchange(groups, counts, slots, base, moved, peak, speed):
    inner, outer, near, far = groups
    kinds = base.shape[0] + moved.shape[0]
    cells = base.shape[1] * base.shape[2]
    width = slots.shape[1]
    dma = pltpu.SemaphoreType.DMA
    sems = []
    for peers in (inner - 1, near - 1, outer * far - 1, 4):
        sems += [dma((peers,)), dma((peers,))]
    return pl.pallas_call(
        functools.partial(exchange_kernel, groups),
        out_shape=(
            jax.ShapeDtypeStruct((4, kinds, width), jnp.float32),
            jax.ShapeDtypeStruct((SUB, LANES), jnp.float32),
        ),
        in_specs=[pl.BlockSpec(memory_space=pltpu.SMEM)] + [pl.BlockSpec(memory_space=pltpu.VMEM)] * 5,
        out_specs=(pl.BlockSpec(memory_space=pltpu.VMEM),) * 2,
        scratch_shapes=[
            pltpu.VMEM((kinds * cells, 2 * LANES), jnp.bfloat16),
            pltpu.VMEM((kinds * cells, TILE), jnp.float32),
            pltpu.VMEM((4, kinds, width), jnp.float32),
            pltpu.VMEM((4, SUB, LANES), jnp.float32),
            pltpu.VMEM((inner - 1, SUB, LANES), jnp.float32),
            pltpu.VMEM((near - 1, SUB, LANES), jnp.float32),
            pltpu.VMEM((outer * far - 1, SUB, LANES), jnp.float32),
        ]
        + sems,
        compiler_params=pltpu.CompilerParams(collective_id=0, has_side_effects=True),
    )(counts, slots, base, moved, peak, speed)


def advance_kernel(top_ref, base_ref, moved_ref, got_ref, state_ref, arrivals_ref):
    peak_acc = jnp.sqrt(jnp.max(top_ref[0:4], axis=(0, 1), keepdims=True))
    peak_speed = jnp.sqrt(jnp.max(top_ref[4:8], axis=(0, 1), keepdims=True))
    step = 0.25 * smooth / (sound_speed + peak_speed + jnp.sqrt(smooth * peak_acc))
    for c in range(2):
        speed = base_ref[2 + c] + step * moved_ref[c]
        state_ref[2 + c] = speed
        state_ref[c] = base_ref[c] + step * speed
        state_ref[5 + c] = moved_ref[c]
    state_ref[4] = base_ref[4] + step * moved_ref[2]
    for d in range(4):
        for c in range(2):
            push = got_ref[d, 6 + c : 7 + c]
            speed = got_ref[d, 2 + c : 3 + c] + step * push
            arrivals_ref[0, 0, d, 2 + c : 3 + c] = speed
            arrivals_ref[0, 0, d, c : c + 1] = got_ref[d, c : c + 1] + step * speed
            arrivals_ref[0, 0, d, 6 + c : 7 + c] = push
        arrivals_ref[0, 0, d, 4:5] = got_ref[d, 4:5] + step * got_ref[d, 8:9]
        arrivals_ref[0, 0, d, 5:6] = got_ref[d, 5:6]


def advance(top, base, moved, got):
    return pl.pallas_call(
        advance_kernel,
        out_shape=(
            jax.ShapeDtypeStruct((7,) + base.shape[1:], jnp.float32),
            jax.ShapeDtypeStruct((1, 1, 4, 8, got.shape[2]), jnp.float32),
        ),
        in_specs=[pl.BlockSpec(memory_space=pltpu.VMEM)] * 4,
        out_specs=(pl.BlockSpec(memory_space=pltpu.VMEM),) * 2,
    )(top, base, moved, got)


def body(
    groups, positions, velocity, density, particle_mass, cell_count, wind_seed, wind_table, migrant_slot, migrant_count
):
    inner, outer, near, far = groups
    cells, base, speed = halo(
        inner * outer, near * far, cell_count.T, positions, velocity, density, particle_mass
    )
    moved, peak = all_forces(wind_table, cells, wind_seed)
    got, top = exchange(groups, migrant_count[0, 0], migrant_slot[0, 0], base, moved, peak, speed)
    return advance(top, base, moved, got)


def solution(mesh):
    shores, crosses = mesh.shape["shore"], mesh.shape["cross"]
    groups = (8, shores // 8, 8, crosses // 8)
    lined = P("shore", "cross", None)
    return jax.shard_map(
        functools.partial(body, groups),
        mesh=mesh,
        in_specs=(
            P(None, "shore", "cross", None),
            P(None, "shore", "cross", None),
            lined,
            lined,
            P("shore", "cross"),
            lined,
            P(),
            P("shore", "cross", None, None),
            lined,
        ),
        out_specs=(P(None, "shore", "cross", None), P("shore", "cross", None, None, None)),
        check_vma=False,
    )
```
